512 devices in a mesh: dp: 128 (over y_lo, x, z), mp: 4 (over y_hi, core).
Axes of the slice: x: 4, y: 4 (y_hi: 2, y_lo: 2; y = y_hi * 2 + y_lo), z: 16, core: 2. Of those that a mesh axis runs over, the one named last changes fastest.
Arguments:
- vlm_tokens: bfloat16 [32768, 2048], P(('dp', 'mp')), may hold values from -64 to 64
- action_tokens: bfloat16 [65536, 2048], P(('dp', 'mp')), may hold values from -64 to 64
- norm_gain: float32 [2048], replicated, may hold values from 0.25 to 1.75
- proj_old: bfloat16 [4096, 4096], P('dp', 'mp'), may hold values from -0.125 to 0.125
Outputs:
- vlm_hidden: bfloat16 [65536, 4096], P('dp', 'mp')
- action_hidden: bfloat16 [65536, 8192], P('dp', 'mp')
- proj_new: bfloat16 [2048, 8192], P('dp', 'mp')
The draws below stay inside these ranges and needn't reach their ends.
All inputs are finite; a program needn't handle non-finite values.
Results may differ from the reference program's by a relative error of at most 0.005.
Values may be sent and summed in bfloat16 or wider, within the bound.
No kernel may reach another device: no remote copies, remote signals or barrier semaphores. Data moves between devices by JAX's collectives and lax.ppermute only.
A program may use at most 64 MiB of HBM per device.

```python
import math
import jax
import jax.numpy as jnp
from jax import lax

D = 2048
FF = 8192
VLM_TOK = 512
ACT_TOK = 512
VLM_ALL = 32768
ACT_ALL = 65536
N_DP = 128
N_MP = 4


def make_tokens(key, number_rows):
    key_base, key_column, key_row = jax.random.split(key, 3)
    entries = jax.random.normal(key_base, (number_rows, D), jnp.float32)
    column = jnp.exp(jax.random.uniform(key_column, (1, D), jnp.float32, math.log(0.3), math.log(3.0)))
    row_scale = jnp.exp(jax.random.uniform(key_row, (number_rows, 1), jnp.float32, 0.0, math.log(10.0)))
    return jnp.clip(entries * column * row_scale, -64.0, 64.0).astype(jnp.bfloat16)


def draw_vlm_tokens(key, part):
    return make_tokens(jax.random.fold_in(key, 11), VLM_ALL)


def draw_action_tokens(key, part):
    return make_tokens(jax.random.fold_in(key, 23), ACT_ALL)


def levels(key, dims, shards, low, top_value):
    level, own = 1.0, jax.random.fold_in(key, 6)
    for dim, parts in shards:
        heights = jnp.exp(jax.random.uniform(jax.random.fold_in(own, dim), (parts,), jnp.float32, low / len(shards), top_value / len(shards)))
        level = level * jnp.repeat(heights, dims[dim] // parts).reshape([-1 if axis == dim else 1 for axis in range(len(dims))])
    return level


def gaussian(key, dims, width, most, cuts=(), kind=jnp.bfloat16):
    factor_of = levels(key, dims, cuts, -0.22, 0.18) if cuts else 1.0
    values = jax.random.normal(key, dims, jnp.float32) * width * factor_of
    return jnp.minimum(jnp.maximum(values, -most), most).astype(kind)


def setup_inputs(seed: int = 0) -> dict:
    key_list = jax.random.split(jax.random.key(seed), 5)
    vlm_tokens = draw_vlm_tokens(jax.random.fold_in(key_list[4], 71), 0)
    action_tokens = draw_action_tokens(jax.random.fold_in(key_list[4], 71), 0)
    norm_gain = jnp.clip(1.0 + 0.15 * jax.random.normal(key_list[2], (D,), jnp.float32), 0.25, 1.75)
    proj_old = gaussian(key_list[3], (2 * D, FF // 2), D ** -0.5, 0.125, ((0, 128), (1, 4)))
    return dict(vlm_tokens=vlm_tokens, action_tokens=action_tokens, norm_gain=norm_gain, proj_old=proj_old)


epsilon = 1e-06

def normalize(row_values, norm_gain):
    values = row_values.astype(jnp.float32)
    factor = lax.rsqrt(lax.optimization_barrier(jnp.mean(values * values, axis=-1, keepdims=True)) + epsilon)
    return (values * factor * norm_gain).astype(jnp.bfloat16)

def reference(vlm_tokens, action_tokens, norm_gain, proj_old):
    groups = N_DP // 2
    row_block = 2 * D // N_DP
    col_block = FF // (2 * N_MP)
    weight = proj_old.reshape(groups, 2, row_block, N_MP, col_block).transpose(0, 2, 3, 1, 4).reshape(D, FF)

    def forward(tokens_block):
        normed = normalize(tokens_block, norm_gain)
        product = jnp.dot(normed, weight, preferred_element_type=jnp.float32)
        return jax.nn.gelu(product, approximate=False).astype(jnp.bfloat16)
    hidden_vlm = lax.map(forward, vlm_tokens.reshape(groups, VLM_TOK, D))
    vlm_hidden = hidden_vlm.reshape(groups, VLM_TOK, N_MP, 2, col_block).transpose(0, 3, 1, 2, 4).reshape(2 * VLM_ALL, FF // 2)
    action_hidden = lax.map(forward, action_tokens.reshape(N_DP, ACT_TOK, D)).reshape(ACT_ALL, FF)
    return (vlm_hidden, action_hidden, weight)
```

```python
import jax
import jax.numpy as jnp
from jax import lax
from jax.sharding import Mesh
from jax.sharding import PartitionSpec as P

ALL = ("y", "x", "k", "b", "h", "c")
NY, NX, NK, NB = 2, 4, 8, 2

epsilon = 1e-06


def normalize(row_values, norm_gain):
    values = row_values.astype(jnp.float32)
    factor = lax.rsqrt(jnp.mean(values * values, axis=-1, keepdims=True) + epsilon)
    return (values * factor * norm_gain).astype(jnp.bfloat16)


def swap(array, axis):
    return lax.ppermute(array, axis, [(0, 1), (1, 0)])


def both(flag, own, other, dim):
    first = jnp.where(flag == 0, own, other)
    second = jnp.where(flag == 0, other, own)
    return jnp.concatenate([first, second], dim)


def spread_rows(proj_old):
    y, b = lax.axis_index("y"), lax.axis_index("b")
    axes = ("y", "b")
    first = lax.ppermute(proj_old, axes, [(0, 2), (3, 1), (2, 3), (1, 0)])
    second = lax.ppermute(proj_old, axes, [(1, 2), (2, 1)])
    own_half = jnp.where(y == b, proj_old, first)
    other_half = jnp.where(y == b, first, second)
    return both(b, own_half, other_half, 1)


def local(vlm_tokens, action_tokens, norm_gain, proj_old):
    b, h, c = (lax.axis_index(a) for a in "bhc")
    row_half = proj_old.shape[0] // 2
    col_block = proj_old.shape[1]
    rows = spread_rows(proj_old)
    gathered = lax.all_gather(rows, ("x", "k", "b"), axis=0, tiled=True)
    weight = gathered.reshape(NX * NK, NB, -1, 2 * col_block).transpose(1, 0, 2, 3).reshape(-1, 2 * col_block)

    kept = lax.dynamic_slice_in_dim(proj_old, b * row_half, row_half, 0)
    given = lax.dynamic_slice_in_dim(proj_old, (1 - b) * row_half, row_half, 0)
    proj_new = both(b, kept, swap(given, "b"), 1)

    vlm = normalize(vlm_tokens, norm_gain)
    action = normalize(action_tokens, norm_gain)
    n_vlm, n_action, width = vlm.shape[0], action.shape[0], vlm.shape[1]
    vlm_pair = jnp.stack([jnp.where(b == 0, vlm, swap(vlm, "b")), jnp.where(b == 0, swap(vlm, "b"), vlm)])
    mine = jnp.concatenate([vlm_pair.reshape(2 * n_vlm, width), action], 0)
    other = swap(mine, "h")
    two = both(h, mine[None], other[None], 0)
    theirs = swap(two, "c")
    four = jnp.stack([jnp.where(c == 0, two, theirs), jnp.where(c == 0, theirs, two)], 1)
    four = four.reshape(4, 2 * n_vlm + n_action, width)
    normed_vlm = four[:, : 2 * n_vlm].reshape(4, 2, n_vlm, width).transpose(1, 0, 2, 3).reshape(-1, width)
    normed_action = four[:, 2 * n_vlm :].reshape(-1, width)

    own_columns = lax.dynamic_slice_in_dim(weight, b * col_block, col_block, 1)
    vlm_total = jnp.dot(normed_vlm, own_columns, preferred_element_type=jnp.float32)
    action_total = jnp.dot(normed_action, weight, preferred_element_type=jnp.float32)
    vlm_hidden = jax.nn.gelu(vlm_total, approximate=False).astype(jnp.bfloat16)
    action_hidden = jax.nn.gelu(action_total, approximate=False).astype(jnp.bfloat16)
    return (vlm_hidden, action_hidden, proj_new)


def solution(mesh):
    finer = Mesh(mesh.devices.reshape(NY, NX, NK, NB, 2, 2), ALL)
    dp, mp = ALL[:4], ALL[4:]
    in_specs = (P(ALL, None), P(ALL, None), P(), P(dp, mp))
    out_specs = (P(dp, mp), P(dp, mp), P(dp, mp))
    return jax.shard_map(local, mesh=finer, in_specs=in_specs, out_specs=out_specs, check_vma=False)
```

```python
import functools

import jax
import jax.numpy as jnp
from jax import lax
from jax.experimental import pallas as pl
from jax.experimental.pallas import tpu as pltpu
from jax.sharding import Mesh
from jax.sharding import PartitionSpec as P

ALL = ("y", "x", "u", "w", "h", "c")
NX, NU, NW = 4, 4, 4
PLANE = ("x", "u", "w", "c")

epsilon = 1e-06


def normalize(row_values, norm_gain):
    values = row_values.astype(jnp.float32)
    factor = lax.rsqrt(jnp.mean(values * values, axis=-1, keepdims=True) + epsilon)
    return (values * factor * norm_gain).astype(jnp.bfloat16)


def swap(array, axis):
    return lax.ppermute(array, axis, [(0, 1), (1, 0)])


def swap_parity(array):
    return lax.ppermute(array, "w", [(i, i ^ 1) for i in range(NW)])


def along(array, x_core, ahead):
    pairs = []
    for x in range(NX):
        for z in range(NU * NW):
            for c in range(2):
                sx, sz = ((x + ahead) % NX, z) if c == x_core else (x, (z + ahead) % (NU * NW))
                pairs.append(((sx * NU * NW + sz) * 2 + c, (x * NU * NW + z) * 2 + c))
    return lax.ppermute(array, PLANE, pairs)


def both(flag, own, other, dim):
    first = jnp.where(flag == 0, own, other)
    second = jnp.where(flag == 0, other, own)
    return jnp.concatenate([first, second], dim)


def in_place(parts, me):
    n = len(parts)
    twice = jnp.stack(parts + parts[:-1])
    return lax.dynamic_slice_in_dim(twice, (n - me) % n, n, 0)


def gather_weight(proj_old):
    y, x, w, c = (lax.axis_index(a) for a in "yxwc")
    half = proj_old.shape[1] // 2
    mine = lax.dynamic_slice_in_dim(proj_old, c * half, half, 1)
    given = lax.dynamic_slice_in_dim(proj_old, (1 - c) * half, half, 1)
    piece = both(c, mine[None], swap(given, "c")[None], 0)
    mates = lax.all_to_all(jnp.broadcast_to(piece, (NU, *piece.shape)), "u", 0, 0)
    planes = both(y, mates[None], swap(mates, "y")[None], 0)
    near = [planes] + [along(planes, 1, d) for d in (1, 2, -1)]
    slab = in_place(near, jnp.where(c == 0, w, x))
    low, high = slab[: slab.shape[0] // 2], slab[slab.shape[0] // 2 :]
    low_prev = along(low, 0, -1)
    high_next = along(high, 0, 1)
    high_prev = along(high, 0, -1)
    low_next = along(low, 0, 1)
    low_far = along(low_prev, 0, -1)
    high_far = along(high_next, 0, 1)
    return low, high, low_next, high_next, low_far, high_far, low_prev, high_prev


def gather_tokens(vlm_tokens, action_tokens, norm_gain):
    b, h, c = lax.axis_index("w") % 2, lax.axis_index("h"), lax.axis_index("c")
    vlm = normalize(vlm_tokens, norm_gain)
    action = normalize(action_tokens, norm_gain)
    n_vlm, width = vlm.shape
    pair = both(b, vlm, swap_parity(vlm), 0)
    mine = jnp.concatenate([pair, action], 0)
    two = both(h, mine[None], swap(mine, "h")[None], 0)
    theirs = swap(two, "c")
    four = jnp.stack([jnp.where(c == 0, two, theirs), jnp.where(c == 0, theirs, two)], 1)
    four = four.reshape(4, -1, width)
    normed_vlm = four[:, : 2 * n_vlm].reshape(4, 2, n_vlm, width).transpose(1, 0, 2, 3).reshape(-1, width)
    return normed_vlm, four[:, 2 * n_vlm :].reshape(-1, width)


def new_projection(proj_old):
    b = lax.axis_index("w") % 2
    row_half = proj_old.shape[0] // 2
    kept = lax.dynamic_slice_in_dim(proj_old, b * row_half, row_half, 0)
    given = lax.dynamic_slice_in_dim(proj_old, (1 - b) * row_half, row_half, 0)
    return both(b, kept, swap_parity(given), 1)


def gelu(total):
    return total * 0.5 * (1.0 + lax.erf(total * 0.7071067811865476))


ROWS = 256


def product_kernel(place, vlm, action, *refs):
    slabs, (vlm_out, action_out, weight, sems) = refs[:8], refs[8:]
    x, w, c, core = (place[i] for i in range(4))
    copies = []
    for r in range(4):
        for s in range(2):
            ref = slabs[2 * r + s]
            for t in range(2):
                q = 2 * s + t
                col = jnp.where(c == 0, lax.rem(x + r, 4), q)
                row = jnp.where(c == 0, q, lax.rem(w + r, 4))
                for y in range(2):
                    copies.append(
                        pltpu.make_async_copy(
                            ref.at[t, y, :, core],
                            weight.at[lax.rem(row, 2), y, col, :, row // 2],
                            sems.at[len(copies)],
                        )
                    )
    for copy in copies:
        copy.start()
    for copy in copies:
        copy.wait()
    depth = action.shape[1]
    half = weight.shape[-1]
    for b in range(2):
        columns = weight[b].reshape(depth, half)
        for i in range(0, action.shape[0], ROWS):
            total = jnp.dot(action[i : i + ROWS, :], columns, preferred_element_type=jnp.float32)
            action_out[i : i + ROWS, b * half : (b + 1) * half] = gelu(total).astype(jnp.bfloat16)
    columns = weight[lax.rem(w, 2)].reshape(depth, half)
    for i in range(0, vlm.shape[0], ROWS):
        total = jnp.dot(vlm[i : i + ROWS, :], columns, preferred_element_type=jnp.float32)
        vlm_out[i : i + ROWS, :] = gelu(total).astype(jnp.bfloat16)


def product(core, vlm, action, slabs):
    x, w, c = (lax.axis_index(a) for a in "xwc")
    place = jnp.stack([x, w, c, core]).astype(jnp.int32)
    half, rows = slabs[0].shape[-1], slabs[0].shape[-2]
    flops = 2 * (vlm.shape[0] + 2 * action.shape[0]) * action.shape[1] * half
    vmem = pl.BlockSpec(memory_space=pltpu.VMEM)
    return pl.pallas_call(
        product_kernel,
        out_shape=(
            jax.ShapeDtypeStruct((vlm.shape[0], half), jnp.bfloat16),
            jax.ShapeDtypeStruct((action.shape[0], 2 * half), jnp.bfloat16),
        ),
        in_specs=[pl.BlockSpec(memory_space=pltpu.SMEM), vmem, vmem] + [pl.BlockSpec(memory_space=pl.ANY)] * 8,
        out_specs=(vmem, vmem),
        scratch_shapes=[
            pltpu.VMEM((2, 2, NX, NU, 2, rows, half), jnp.bfloat16),
            pltpu.SemaphoreType.DMA((32,)),
        ],
        compiler_params=pltpu.CompilerParams(vmem_limit_bytes=40 * 1024 * 1024),
        cost_estimate=pl.CostEstimate(flops=flops, bytes_accessed=12 * 1024 * 1024, transcendentals=0),
        name="product",
    )(place, vlm, action, *slabs)


def local(vlm_tokens, action_tokens, norm_gain, proj_old):
    c = lax.axis_index("c")
    slabs = gather_weight(proj_old)
    vlm, action = gather_tokens(vlm_tokens, action_tokens, norm_gain)
    vlm_given, action_given = product(1 - c, vlm, action, slabs)
    vlm_own, action_own = product(c, vlm, action, slabs)
    n, half = vlm_own.shape
    vlm_taken, action_taken = swap(vlm_given, "c"), swap(action_given, "c")
    vlm_hidden = both(c, vlm_own, vlm_taken, 1)
    action_own, action_taken = action_own.reshape(-1, 2, half), action_taken.reshape(-1, 2, half)
    action_hidden = both(c, action_own, action_taken, 2).reshape(-1, 4 * half)
    return (vlm_hidden, action_hidden, new_projection(proj_old))


def solution(mesh):
    finer = Mesh(mesh.devices.reshape(2, NX, NU, NW, 2, 2), ALL)
    dp, mp = ALL[:4], ALL[4:]
    in_specs = (P(ALL, None), P(ALL, None), P(), P(dp, mp))
    out_specs = (P(dp, mp), P(dp, mp), P(dp, mp))
    return jax.shard_map(local, mesh=finer, in_specs=in_specs, out_specs=out_specs, check_vma=False)
```

```python
import jax
import jax.numpy as jnp
from jax import lax
from jax.experimental import pallas as pl
from jax.experimental.pallas import tpu as pltpu
from jax.sharding import Mesh
from jax.sharding import PartitionSpec as P


ALL = ("y", "x", "u", "w", "h", "c")
NX, NU, NW = 4, 4, 4
PLANE = ("x", "u", "w", "c")

epsilon = 1e-06


def normalize(row_values, norm_gain):
    values = row_values.astype(jnp.float32)
    factor = lax.rsqrt(jnp.mean(values * values, axis=-1, keepdims=True) + epsilon)
    return (values * factor * norm_gain).astype(jnp.bfloat16)


def swap(array, axis):
    return lax.ppermute(array, axis, [(0, 1), (1, 0)])


def swap_parity(array):
    return lax.ppermute(array, "w", [(i, i ^ 1) for i in range(NW)])


def along(array, x_core, ahead):
    pairs = []
    for x in range(NX):
        for z in range(NU * NW):
            for c in range(2):
                sx, sz = ((x + ahead) % NX, z) if c == x_core else (x, (z + ahead) % (NU * NW))
                pairs.append(((sx * NU * NW + sz) * 2 + c, (x * NU * NW + z) * 2 + c))
    return lax.ppermute(array, PLANE, pairs)


def both(flag, own, other, dim):
    first = jnp.where(flag == 0, own, other)
    second = jnp.where(flag == 0, other, own)
    return jnp.concatenate([first, second], dim)


def in_place(parts, me):
    n = len(parts)
    twice = jnp.stack(parts + parts[:-1])
    return lax.dynamic_slice_in_dim(twice, (n - me) % n, n, 0)


def near_weight(proj_old):
    y, x, w, c = (lax.axis_index(a) for a in "yxwc")
    half = proj_old.shape[1] // 2
    mine = lax.dynamic_slice_in_dim(proj_old, c * half, half, 1)
    given = lax.dynamic_slice_in_dim(proj_old, (1 - c) * half, half, 1)
    piece = both(c, mine[None], swap(given, "c")[None], 0)
    far = [piece] + [lax.ppermute(piece, "u", [((i + d) % NU, i) for i in range(NU)]) for d in (2, 1, 3)]
    far[1], far[2] = far[2], far[1]
    mates = in_place(far, lax.axis_index("u"))
    other = swap(mates, "y")
    planes = both(y, mates[None], other[None], 0)
    near = [planes] + [along(planes, 1, d) for d in (1, 2, -1)]
    return in_place(near, jnp.where(c == 0, w, x))


def all_weight(slab):
    low, high = slab[: slab.shape[0] // 2], slab[slab.shape[0] // 2 :]
    low_prev = along(low, 0, -1)
    high_next = along(high, 0, 1)
    high_prev = along(high, 0, -1)
    low_next = along(low, 0, 1)
    low_far = along(low_prev, 0, -1)
    high_far = along(high_next, 0, 1)
    return (low, high, low_next, high_next, low_far, high_far, low_prev, high_prev)


def chip_tokens(vlm_tokens, action_tokens, norm_gain):
    vlm = normalize(vlm_tokens, norm_gain)
    action = normalize(action_tokens, norm_gain)
    other = swap_parity(vlm)
    pair = both(lax.axis_index("w") % 2, vlm, other, 0)
    return jnp.concatenate([pair, action], 0)


def all_tokens(mine, n_vlm):
    h, c = lax.axis_index("h"), lax.axis_index("c")
    width = mine.shape[1]
    other = swap(mine, "h")
    two = both(h, mine[None], other[None], 0)
    theirs = swap(two, "c")
    four = jnp.stack([jnp.where(c == 0, two, theirs), jnp.where(c == 0, theirs, two)], 1)
    four = four.reshape(4, -1, width)
    normed_vlm = four[:, : 2 * n_vlm].reshape(4, 2, n_vlm, width).transpose(1, 0, 2, 3).reshape(-1, width)
    return normed_vlm, four[:, 2 * n_vlm :].reshape(-1, width)


def new_projection(proj_old):
    b = lax.axis_index("w") % 2
    row_half = proj_old.shape[0] // 2
    kept = lax.dynamic_slice_in_dim(proj_old, b * row_half, row_half, 0)
    given = lax.dynamic_slice_in_dim(proj_old, (1 - b) * row_half, row_half, 0)
    return both(b, kept, swap_parity(given), 1)


def gelu(total):
    return total * 0.5 * (1.0 + lax.erf(total * 0.7071067811865476))


ROWS = 256


def products(place, core, vlm, action, slabs, weight, sems, store):
    x, w, c = (place[i] for i in range(3))
    copies = []
    for r in range(4):
        for s in range(2):
            ref = slabs[2 * r + s]
            for t in range(2):
                q = 2 * s + t
                col = jnp.where(c == 0, lax.rem(x + r, 4), q)
                row = jnp.where(c == 0, q, lax.rem(w + r, 4))
                for y in range(2):
                    copies.append(
                        pltpu.make_async_copy(
                            ref.at[t, y, :, core],
                            weight.at[lax.rem(row, 2), y, col, :, row // 2],
                            sems.at[len(copies)],
                        )
                    )
    for copy in copies:
        copy.start()
    for copy in copies:
        copy.wait()
    depth, half = action.shape[1], weight.shape[-1]
    for block in range(3):
        rows, parity = (action, block) if block < 2 else (vlm, lax.rem(w, 2))
        columns = weight[parity].reshape(depth, half)
        for i in range(0, rows.shape[0], ROWS):
            total = jnp.dot(rows[i : i + ROWS, :], columns, preferred_element_type=jnp.float32)
            store(block, i, gelu(total).astype(jnp.bfloat16))


def given_kernel(place, vlm, action, *refs):
    slabs, (out, weight, sems) = refs[:8], refs[8:]

    def store(block, i, values):
        out[block, i : i + ROWS, :] = values

    products(place, 1 - place[2], vlm, action, slabs, weight, sems, store)


def column_copies(core, parts, vlm_out, action_out, sems):
    half = parts.shape[-1]
    b_copies = [
        pltpu.make_async_copy(
            parts.at[b], action_out.at[:, pl.ds(pl.multiple_of((2 * b + core) * half, half), half)], sems.at[b]
        )
        for b in range(2)
    ]
    vlm_copy = pltpu.make_async_copy(
        parts.at[2], vlm_out.at[:, pl.ds(pl.multiple_of(core * half, half), half)], sems.at[2]
    )
    return b_copies + [vlm_copy]


def own_kernel(place, vlm, action, *refs):
    slabs, (vlm_out, action_out, weight, stage, sems, out_sems) = refs[:8], refs[8:]
    outs = column_copies(place[2], stage, vlm_out, action_out, out_sems)

    def store(block, i, values):
        stage[block, i : i + ROWS, :] = values
        if i + ROWS == stage.shape[1]:
            outs[block].start()

    products(place, place[2], vlm, action, slabs, weight, sems, store)
    for copy in outs:
        copy.wait()


def merge_kernel(place, parts, vlm_in, action_in, vlm_out, action_out, sems):
    del vlm_in, action_in
    copies = column_copies(1 - place[2], parts, vlm_out, action_out, sems)
    for copy in copies:
        copy.start()
    for copy in copies:
        copy.wait()


SMEM = pl.BlockSpec(memory_space=pltpu.SMEM)
VMEM = pl.BlockSpec(memory_space=pltpu.VMEM)
HBM = pl.BlockSpec(memory_space=pltpu.HBM)


def outputs(vlm, action, slabs):
    place = jnp.stack([lax.axis_index(a) for a in "xwc"]).astype(jnp.int32)
    half, rows, count = slabs[0].shape[-1], slabs[0].shape[-2], action.shape[0]
    cost = pl.CostEstimate(
        flops=6 * count * action.shape[1] * half, bytes_accessed=12 * 1024 * 1024, transcendentals=0
    )
    params = pltpu.CompilerParams(vmem_limit_bytes=20 * 1024 * 1024)
    weight = pltpu.VMEM((2, 2, NX, NU, 2, rows, half), jnp.bfloat16)
    sems = pltpu.SemaphoreType.DMA((32,))
    parts = jax.ShapeDtypeStruct((3, count, half), jnp.bfloat16)
    wide = (
        jax.ShapeDtypeStruct((count, 2 * half), jnp.bfloat16),
        jax.ShapeDtypeStruct((count, 4 * half), jnp.bfloat16),
    )
    given = pl.pallas_call(
        given_kernel,
        out_shape=parts,
        in_specs=[SMEM, VMEM, VMEM] + [HBM] * 8,
        out_specs=VMEM,
        scratch_shapes=[weight, sems],
        compiler_params=params,
        cost_estimate=cost,
        name="given",
    )(place, vlm, action, *slabs)
    own = pl.pallas_call(
        own_kernel,
        out_shape=wide,
        in_specs=[SMEM, VMEM, VMEM] + [HBM] * 8,
        out_specs=(HBM, HBM),
        scratch_shapes=[weight, pltpu.VMEM(parts.shape, parts.dtype), sems, pltpu.SemaphoreType.DMA((3,))],
        compiler_params=params,
        cost_estimate=cost,
        name="own",
    )(place, vlm, action, *slabs)
    taken = swap(given, "c")
    return pl.pallas_call(
        merge_kernel,
        out_shape=wide,
        in_specs=[SMEM, HBM, HBM, HBM],
        out_specs=(HBM, HBM),
        scratch_shapes=[pltpu.SemaphoreType.DMA((3,))],
        input_output_aliases={2: 0, 3: 1},
        name="merge",
    )(place, taken, *own)


def local(vlm_tokens, action_tokens, norm_gain, proj_old):
    slab, mine = near_weight(proj_old), chip_tokens(vlm_tokens, action_tokens, norm_gain)
    slab, mine = lax.optimization_barrier((slab, mine))
    slabs = all_weight(slab)
    vlm, action = all_tokens(mine, vlm_tokens.shape[0])
    vlm_hidden, action_hidden = outputs(vlm, action, slabs)
    return (vlm_hidden, action_hidden, new_projection(proj_old))


def solution(mesh):
    finer = Mesh(mesh.devices.reshape(2, NX, NU, NW, 2, 2), ALL)
    dp, mp = ALL[:4], ALL[4:]
    in_specs = (P(ALL, None), P(ALL, None), P(), P(dp, mp))
    out_specs = (P(dp, mp), P(dp, mp), P(dp, mp))
    return jax.shard_map(local, mesh=finer, in_specs=in_specs, out_specs=out_specs, check_vma=False)
```

```python
import jax
import jax.numpy as jnp
from jax import lax
from jax.experimental import pallas as pl
from jax.experimental.pallas import tpu as pltpu
from jax.sharding import Mesh
from jax.sharding import PartitionSpec as P


ALL = ("y", "x", "u", "w", "h", "c")
NX, NU, NW = 4, 4, 4
PLANE = ("x", "u", "w", "c")

epsilon = 1e-06


def normalize(row_values, norm_gain):
    values = row_values.astype(jnp.float32)
    factor = lax.rsqrt(jnp.mean(values * values, axis=-1, keepdims=True) + epsilon)
    return (values * factor * norm_gain).astype(jnp.bfloat16)


def swap(array, axis):
    return lax.ppermute(array, axis, [(0, 1), (1, 0)])


def swap_parity(array):
    return lax.ppermute(array, "w", [(i, i ^ 1) for i in range(NW)])


def along(array, x_core, ahead):
    pairs = []
    for x in range(NX):
        for z in range(NU * NW):
            for c in range(2):
                sx, sz = ((x + ahead) % NX, z) if c == x_core else (x, (z + ahead) % (NU * NW))
                pairs.append(((sx * NU * NW + sz) * 2 + c, (x * NU * NW + z) * 2 + c))
    return lax.ppermute(array, PLANE, pairs)


def both(flag, own, other, dim):
    first = jnp.where(flag == 0, own, other)
    second = jnp.where(flag == 0, other, own)
    return jnp.concatenate([first, second], dim)


def near_weight(proj_old):
    c = lax.axis_index("c")
    half = proj_old.shape[1] // 2
    mine = lax.dynamic_slice_in_dim(proj_old, c * half, half, 1)
    given = lax.dynamic_slice_in_dim(proj_old, (1 - c) * half, half, 1)
    taken = swap(given, "c")
    mates = lax.all_gather(jnp.stack([mine, taken]), "u")
    planes = lax.all_gather(mates, "y")
    return [planes] + [along(planes, 1, d) for d in (1, 2, -1)]


def all_weight(pieces):
    low, high = lax.optimization_barrier((jnp.stack(pieces[:2]), jnp.stack(pieces[2:])))
    low_prev = along(low, 0, -1)
    high_next = along(high, 0, 1)
    high_prev = along(high, 0, -1)
    low_next = along(low, 0, 1)
    low_far = along(low_prev, 0, -1)
    high_far = along(high_next, 0, 1)
    return (low, high, low_next, high_next, low_far, high_far, low_prev, high_prev)


def chip_tokens(vlm_tokens, action_tokens, norm_gain):
    vlm = normalize(vlm_tokens, norm_gain)
    action = normalize(action_tokens, norm_gain)
    other = swap_parity(vlm)
    pair = both(lax.axis_index("w") % 2, vlm, other, 0)
    return jnp.concatenate([pair, action], 0)


def all_tokens(mine, n_vlm):
    h, c = lax.axis_index("h"), lax.axis_index("c")
    width = mine.shape[1]
    other = swap(mine, "h")
    two = both(h, mine[None], other[None], 0)
    theirs = swap(two, "c")
    four = jnp.stack([jnp.where(c == 0, two, theirs), jnp.where(c == 0, theirs, two)], 1)
    four = four.reshape(4, -1, width)
    normed_vlm = four[:, : 2 * n_vlm].reshape(4, 2, n_vlm, width).transpose(1, 0, 2, 3).reshape(-1, width)
    return normed_vlm, four[:, 2 * n_vlm :].reshape(-1, width)


def new_projection(proj_old):
    b = lax.axis_index("w") % 2
    row_half = proj_old.shape[0] // 2
    kept = lax.dynamic_slice_in_dim(proj_old, b * row_half, row_half, 0)
    given = lax.dynamic_slice_in_dim(proj_old, (1 - b) * row_half, row_half, 0)
    return both(b, kept, swap_parity(given), 1)


def gelu(total):
    return total * 0.5 * (1.0 + lax.erf(total * 0.7071067811865476))


ROWS = 256


def products(place, core, vlm, action, slabs, weight, sems, store):
    x, w, c = (place[i] for i in range(3))
    copies = []
    for r in range(4):
        for s in range(2):
            ref = slabs[2 * r + s]
            for t in range(2):
                q = 2 * s + t
                col = lax.rem(x + jnp.where(c == 0, r, q), NX)
                row = lax.rem(w + jnp.where(c == 0, q, r), NW)
                for y in range(2):
                    copies.append(
                        pltpu.make_async_copy(
                            ref.at[t, y, :, core],
                            weight.at[lax.rem(row, 2), y, col, :, row // 2],
                            sems.at[len(copies)],
                        )
                    )
    for copy in copies:
        copy.start()
    for copy in copies:
        copy.wait()
    depth, half = action.shape[1], weight.shape[-1]
    for block in range(3):
        rows, parity = (action, block) if block < 2 else (vlm, lax.rem(w, 2))
        columns = weight[parity].reshape(depth, half)
        for i in range(0, rows.shape[0], ROWS):
            total = jnp.dot(rows[i : i + ROWS, :], columns, preferred_element_type=jnp.float32)
            store(block, i, gelu(total).astype(jnp.bfloat16))


def given_kernel(place, vlm, action, *refs):
    slabs, (out, weight, sems) = refs[:8], refs[8:]

    def store(block, i, values):
        out[block, i : i + ROWS, :] = values

    products(place, 1, vlm, action, slabs, weight, sems, store)


def column_copies(core, parts, vlm_out, action_out, sems):
    half = parts.shape[-1]
    b_copies = [
        pltpu.make_async_copy(
            parts.at[b], action_out.at[:, pl.ds(pl.multiple_of((2 * b + core) * half, half), half)], sems.at[b]
        )
        for b in range(2)
    ]
    vlm_copy = pltpu.make_async_copy(
        parts.at[2], vlm_out.at[:, pl.ds(pl.multiple_of(core * half, half), half)], sems.at[2]
    )
    return b_copies + [vlm_copy]


def own_kernel(place, vlm, action, *refs):
    slabs, (vlm_out, action_out, weight, stage, sems, out_sems) = refs[:8], refs[8:]
    outs = column_copies(place[2], stage, vlm_out, action_out, out_sems)

    def store(block, i, values):
        stage[block, i : i + ROWS, :] = values
        if i + ROWS == stage.shape[1]:
            outs[block].start()

    products(place, 0, vlm, action, slabs, weight, sems, store)
    for copy in outs:
        copy.wait()


def merge_kernel(place, parts, vlm_in, action_in, vlm_out, action_out, sems):
    del vlm_in, action_in
    copies = column_copies(1 - place[2], parts, vlm_out, action_out, sems)
    for copy in copies:
        copy.start()
    for copy in copies:
        copy.wait()


SMEM = pl.BlockSpec(memory_space=pltpu.SMEM)
VMEM = pl.BlockSpec(memory_space=pltpu.VMEM)
HBM = pl.BlockSpec(memory_space=pltpu.HBM)


def outputs(vlm, action, slabs):
    place = jnp.stack([lax.axis_index(a) for a in "xwc"]).astype(jnp.int32)
    half, rows, count = slabs[0].shape[-1], slabs[0].shape[-2], action.shape[0]
    cost = pl.CostEstimate(
        flops=6 * count * action.shape[1] * half, bytes_accessed=12 * 1024 * 1024, transcendentals=0
    )
    params = pltpu.CompilerParams(vmem_limit_bytes=12 * 1024 * 1024)
    weight = pltpu.VMEM((2, 2, NX, NU, 2, rows, half), jnp.bfloat16)
    sems = pltpu.SemaphoreType.DMA((32,))
    parts = jax.ShapeDtypeStruct((3, count, half), jnp.bfloat16)
    wide = (
        jax.ShapeDtypeStruct((count, 2 * half), jnp.bfloat16),
        jax.ShapeDtypeStruct((count, 4 * half), jnp.bfloat16),
    )
    given = pl.pallas_call(
        given_kernel,
        out_shape=parts,
        in_specs=[SMEM, VMEM, VMEM] + [HBM] * 8,
        out_specs=VMEM,
        scratch_shapes=[weight, sems],
        compiler_params=params,
        cost_estimate=cost,
        name="given",
    )(place, vlm, action, *slabs)
    own = pl.pallas_call(
        own_kernel,
        out_shape=wide,
        in_specs=[SMEM, VMEM, VMEM] + [HBM] * 8,
        out_specs=(HBM, HBM),
        scratch_shapes=[weight, pltpu.VMEM(parts.shape, parts.dtype), sems, pltpu.SemaphoreType.DMA((3,))],
        compiler_params=params,
        cost_estimate=cost,
        name="own",
    )(place, vlm, action, *slabs)
    taken = swap(given, "c")
    return pl.pallas_call(
        merge_kernel,
        out_shape=wide,
        in_specs=[SMEM, VMEM, HBM, HBM],
        out_specs=(HBM, HBM),
        scratch_shapes=[pltpu.SemaphoreType.DMA((3,))],
        input_output_aliases={2: 0, 3: 1},
        name="merge",
    )(place, taken, *own)


def local(vlm_tokens, action_tokens, norm_gain, proj_old):
    pieces = near_weight(proj_old)
    mine = chip_tokens(vlm_tokens, action_tokens, norm_gain)
    slabs = all_weight(pieces)
    vlm, action = all_tokens(mine, vlm_tokens.shape[0])
    vlm_hidden, action_hidden = outputs(vlm, action, slabs)
    new = new_projection(proj_old)
    return (vlm_hidden, action_hidden, new)


def solution(mesh):
    finer = Mesh(mesh.devices.reshape(2, NX, NU, NW, 2, 2), ALL)
    dp, mp = ALL[:4], ALL[4:]
    in_specs = (P(ALL, None), P(ALL, None), P(), P(dp, mp))
    out_specs = (P(dp, mp), P(dp, mp), P(dp, mp))
    return jax.shard_map(local, mesh=finer, in_specs=in_specs, out_specs=out_specs, check_vma=False)
```

```python
import functools

import jax
import jax.numpy as jnp
from jax import lax
from jax.experimental import pallas as pl
from jax.experimental.pallas import tpu as pltpu
from jax.sharding import Mesh
from jax.sharding import PartitionSpec as P


ALL = ("y", "x", "u", "w", "h", "c")
NX, NU, NW = 4, 4, 4
PLANE = ("x", "u", "w", "c")

epsilon = 1e-06


def normalize(row_values, norm_gain):
    values = row_values.astype(jnp.float32)
    factor = lax.rsqrt(jnp.mean(values * values, axis=-1, keepdims=True) + epsilon)
    return (values * factor * norm_gain).astype(jnp.bfloat16)


def swap(array, axis):
    return lax.ppermute(array, axis, [(0, 1), (1, 0)])


def swap_parity(array):
    return lax.ppermute(array, "w", [(i, i ^ 1) for i in range(NW)])


def along(array, x_core, ahead):
    pairs = []
    for x in range(NX):
        for z in range(NU * NW):
            for c in range(2):
                sx, sz = ((x + ahead) % NX, z) if c == x_core else (x, (z + ahead) % (NU * NW))
                pairs.append(((sx * NU * NW + sz) * 2 + c, (x * NU * NW + z) * 2 + c))
    return lax.ppermute(array, PLANE, pairs)


def both(flag, own, other, dim):
    first = jnp.where(flag == 0, own, other)
    second = jnp.where(flag == 0, other, own)
    return jnp.concatenate([first, second], dim)


def near_weight(proj_old):
    c = lax.axis_index("c")
    half = proj_old.shape[1] // 2
    mine = lax.dynamic_slice_in_dim(proj_old, c * half, half, 1)
    given = lax.dynamic_slice_in_dim(proj_old, (1 - c) * half, half, 1)
    taken = swap(given, "c")
    mates = lax.all_gather(jnp.stack([mine, taken]), "u")
    planes = lax.all_gather(mates, "y")
    after, before = along(planes, 1, 1), along(planes, 1, -1)
    opposite = [along(planes[:1], 1, 2), along(planes[1:], 1, -2)]
    return [planes, after, jnp.concatenate(opposite, 0), before]


def all_weight(pieces):
    part = pieces[0].shape[-1] // 2
    parts = [jnp.stack([p[..., i * part : (i + 1) * part] for p in pieces]) for i in range(2)]
    parts = lax.optimization_barrier(parts)
    near = []
    for i in range(2):
        before = along(parts[i], 0, -1)
        after = along(parts[i], 0, 1)
        near.append((after, before))
    slabs = []
    for i in range(2):
        after, before = near[i]
        half = before.shape[0] // 2
        first = along(before[:half], 0, -1)
        last = along(after[half:], 0, 1)
        slabs.append((parts[i], after, before, first, last))
    return slabs


def chip_tokens(vlm_tokens, action_tokens, norm_gain):
    vlm = normalize(vlm_tokens, norm_gain)
    action = normalize(action_tokens, norm_gain)
    other = swap_parity(vlm)
    pair = both(lax.axis_index("w") % 2, vlm, other, 0)
    return jnp.concatenate([pair, action], 0)


def all_tokens(mine, n_vlm):
    h, c = lax.axis_index("h"), lax.axis_index("c")
    width = mine.shape[1]
    other = swap(mine, "h")
    two = both(h, mine[None], other[None], 0)
    theirs = swap(two, "c")
    four = jnp.stack([jnp.where(c == 0, two, theirs), jnp.where(c == 0, theirs, two)], 1)
    four = four.reshape(4, -1, width)
    normed_vlm = four[:, : 2 * n_vlm].reshape(4, 2, n_vlm, width).transpose(1, 0, 2, 3).reshape(-1, width)
    return normed_vlm, four[:, 2 * n_vlm :].reshape(-1, width)


def new_projection(proj_old):
    b = lax.axis_index("w") % 2
    row_half = proj_old.shape[0] // 2
    kept = lax.dynamic_slice_in_dim(proj_old, b * row_half, row_half, 0)
    given = lax.dynamic_slice_in_dim(proj_old, (1 - b) * row_half, row_half, 0)
    taken = swap_parity(given)
    return both(b, kept, taken, 1)


def gelu(total):
    return total * 0.5 * (1.0 + lax.erf(total * 0.7071067811865476))


ROWS = 256
SLABS = ((0, range(4), 0), (1, range(4), 0), (3, range(4), 0), (2, range(2), 0), (2, range(2, 4), 2))


def weight_copies(place, core, slabs, weight, sems):
    x, w, c = (place[i] for i in range(3))
    part = slabs[0].shape[-1]
    copies = []
    for ref, (r, pieces, start) in zip(slabs, SLABS):
        for q in pieces:
            col = lax.rem(x + jnp.where(c == 0, r, q), NX)
            row = lax.rem(w + jnp.where(c == 0, q, r), NW)
            columns = pl.ds(pl.multiple_of(lax.rem(row, 2) * part, part), part)
            for y in range(2):
                copies.append(
                    pltpu.make_async_copy(
                        ref.at[q - start, y, :, core],
                        weight.at[y, col, :, row // 2, :, columns],
                        sems.at[len(copies)],
                    )
                )
    return copies


def products(place, vlm, action, weight, store):
    depth, part = action.shape[1], weight.shape[-1] // 2
    columns = weight[...].reshape(depth, 2 * part)
    for i in range(0, action.shape[0], ROWS):
        total = jnp.dot(action[i : i + ROWS, :], columns, preferred_element_type=jnp.float32)
        values = gelu(total).astype(jnp.bfloat16)
        store(0, i, values[:, :part])
        store(1, i, values[:, part:])
    columns = weight[..., pl.ds(pl.multiple_of(lax.rem(place[1], 2) * part, part), part)].reshape(depth, part)
    for i in range(0, vlm.shape[0], ROWS):
        total = jnp.dot(vlm[i : i + ROWS, :], columns, preferred_element_type=jnp.float32)
        store(2, i, gelu(total).astype(jnp.bfloat16))


def column_copies(number, core, parts, vlm_out, action_out, sems):
    part = parts.shape[-1]
    starts = [pl.multiple_of((4 * b + 2 * core + number) * part, part) for b in (0, 1, 0)]
    return [
        pltpu.make_async_copy(parts.at[i], out.at[:, pl.ds(starts[i], part)], sems.at[i])
        for i, out in enumerate((action_out, action_out, vlm_out))
    ]


def part_kernel(number, given, own, n_in, place, vlm, action, *refs):
    slabs, refs = refs[: len(SLABS)], list(refs[n_in:])
    given_out = refs.pop(0) if given else None
    vlm_out, action_out = (refs.pop(0), refs.pop(0)) if own else (None, None)
    weights, stage, sems, out_sems = refs
    jobs = [1] * given + [0] * own
    copies = [weight_copies(place, core, slabs, weights.at[n], sems.at[n]) for n, core in enumerate(jobs)]
    for job in copies:
        for copy in job:
            copy.start()
    for n, core in enumerate(jobs):
        for copy in copies[n]:
            copy.wait()
        target = given_out if core else stage
        outs = [] if core else column_copies(number, place[2], stage, vlm_out, action_out, out_sems)

        def store(block, i, values, target=target, outs=outs):
            target[block, i : i + ROWS, :] = values
            if outs and i + ROWS == target.shape[1]:
                outs[block].start()

        products(place, vlm, action, weights.at[n], store)
        for copy in outs:
            copy.wait()


def merge_kernel(place, first, second, vlm_in, action_in, vlm_out, action_out, sems):
    del vlm_in, action_in
    copies = []
    for number, parts in enumerate((first, second)):
        copies += column_copies(number, 1 - place[2], parts, vlm_out, action_out, sems.at[number])
    for copy in copies:
        copy.start()
    for copy in copies:
        copy.wait()


SMEM = pl.BlockSpec(memory_space=pltpu.SMEM)
VMEM = pl.BlockSpec(memory_space=pltpu.VMEM)
HBM = pl.BlockSpec(memory_space=pltpu.HBM)


def outputs(vlm, action, slabs):
    place = jnp.stack([lax.axis_index(a) for a in "xwc"]).astype(jnp.int32)
    part, rows, count, depth = slabs[0][0].shape[-1], slabs[0][0].shape[-2], *action.shape
    taken = jax.ShapeDtypeStruct((3, count, part), jnp.bfloat16)
    wide = tuple(jax.ShapeDtypeStruct((count, n * part), jnp.bfloat16) for n in (4, 8))

    def call(number, given, own, before=()):
        jobs = given + own
        n_in = len(SLABS) + len(before)
        kernel = functools.partial(part_kernel, number, given, own, n_in)
        return pl.pallas_call(
            kernel,
            out_shape=(taken,) * given + wide * own,
            in_specs=[SMEM, VMEM, VMEM] + [HBM] * n_in,
            out_specs=(VMEM,) * given + (HBM, HBM) * own,
            scratch_shapes=[
                pltpu.VMEM((jobs, 2, NX, NU, 2, rows, 2 * part), jnp.bfloat16),
                pltpu.VMEM(taken.shape, taken.dtype),
                pltpu.SemaphoreType.DMA((jobs, 32)),
                pltpu.SemaphoreType.DMA((3,)),
            ],
            input_output_aliases={3 + len(SLABS) + i: given + i for i in range(len(before))},
            compiler_params=pltpu.CompilerParams(vmem_limit_bytes=14 * 1024 * 1024),
            cost_estimate=pl.CostEstimate(
                flops=6 * count * depth * part * jobs, bytes_accessed=6 * 1024 * 1024, transcendentals=0
            ),
        )(place, vlm, action, *slabs[number], *before)

    given_low, *wide_low = call(0, 1, 1)
    taken_low = swap(given_low, "c")
    (given_high,) = call(1, 1, 0)
    taken_high = swap(given_high, "c")
    wide_own = call(1, 0, 1, tuple(wide_low))
    return pl.pallas_call(
        merge_kernel,
        out_shape=wide,
        in_specs=[SMEM, VMEM, VMEM, HBM, HBM],
        out_specs=(HBM, HBM),
        scratch_shapes=[pltpu.SemaphoreType.DMA((2, 3))],
        input_output_aliases={3: 0, 4: 1},
        name="merge",
    )(place, taken_low, taken_high, *wide_own)


def local(vlm_tokens, action_tokens, norm_gain, proj_old):
    pieces = near_weight(proj_old)
    mine = chip_tokens(vlm_tokens, action_tokens, norm_gain)
    slabs = all_weight(pieces)
    vlm, action = all_tokens(mine, vlm_tokens.shape[0])
    vlm_hidden, action_hidden = outputs(vlm, action, slabs)
    return (vlm_hidden, action_hidden, new_projection(proj_old))


def solution(mesh):
    finer = Mesh(mesh.devices.reshape(2, NX, NU, NW, 2, 2), ALL)
    dp, mp = ALL[:4], ALL[4:]
    in_specs = (P(ALL, None), P(ALL, None), P(), P(dp, mp))
    out_specs = (P(dp, mp), P(dp, mp), P(dp, mp))
    return jax.shard_map(local, mesh=finer, in_specs=in_specs, out_specs=out_specs, check_vma=False)
```

```python
import functools

import jax
import jax.numpy as jnp
from jax import lax
from jax.experimental import pallas as pl
from jax.experimental.pallas import tpu as pltpu
from jax.sharding import Mesh
from jax.sharding import PartitionSpec as P


ALL = ("y", "x", "u", "w", "h", "c")
NX, NU, NW = 4, 4, 4
PLANE = ("x", "u", "w", "c")

epsilon = 1e-06


def normalize(row_values, norm_gain):
    values = row_values.astype(jnp.float32)
    factor = lax.rsqrt(jnp.mean(values * values, axis=-1, keepdims=True) + epsilon)
    return (values * factor * norm_gain).astype(jnp.bfloat16)


def swap(array, axis):
    return lax.ppermute(array, axis, [(0, 1), (1, 0)])


def swap_parity(array):
    return lax.ppermute(array, "w", [(i, i ^ 1) for i in range(NW)])


def along(array, x_core, ahead):
    pairs = []
    for x in range(NX):
        for z in range(NU * NW):
            for c in range(2):
                sx, sz = ((x + ahead) % NX, z) if c == x_core else (x, (z + ahead) % (NU * NW))
                pairs.append(((sx * NU * NW + sz) * 2 + c, (x * NU * NW + z) * 2 + c))
    return lax.ppermute(array, PLANE, pairs)


def both(flag, own, other, dim):
    first = jnp.where(flag == 0, own, other)
    second = jnp.where(flag == 0, other, own)
    return jnp.concatenate([first, second], dim)


def near_weight(proj_old):
    c = lax.axis_index("c")
    half = proj_old.shape[1] // 2
    mine = lax.dynamic_slice_in_dim(proj_old, c * half, half, 1)
    given = lax.dynamic_slice_in_dim(proj_old, (1 - c) * half, half, 1)
    taken = swap(given, "c")
    mates = lax.all_gather(jnp.stack([mine, taken]), "u")
    planes = lax.all_gather(mates, "y")
    after, before = along(planes, 1, 1), along(planes, 1, -1)
    opposite = [along(planes[:1], 1, 2), along(planes[1:], 1, -2)]
    return [planes, after, jnp.concatenate(opposite, 0), before]


def all_weight(pieces):
    part = pieces[0].shape[-1] // 2
    low, high = (jnp.stack([p[..., i * part : (i + 1) * part] for p in pieces]) for i in range(2))
    low, high = lax.optimization_barrier((low, high))
    low_before = along(low, 0, -1)
    low_after = along(low, 0, 1)
    high_before = along(high, 0, -1)
    high_after = along(high, 0, 1)
    low_far = along(low_before, 0, -1)
    high_far = along(high_after, 0, 1)
    return (low, low_after, low_far, low_before), (high, high_after, high_far, high_before)


def pair_exchange(vlm_tokens, action_tokens, norm_gain, proj_old):
    b = lax.axis_index("w") % 2
    row_half, width = proj_old.shape[0] // 2, vlm_tokens.shape[1]
    vlm = normalize(vlm_tokens, norm_gain)
    action = normalize(action_tokens, norm_gain)
    kept = lax.dynamic_slice_in_dim(proj_old, b * row_half, row_half, 0)
    given = lax.dynamic_slice_in_dim(proj_old, (1 - b) * row_half, row_half, 0)
    folds = width // given.shape[1]
    given = jnp.concatenate(jnp.split(given, folds, 0), 1)
    other = swap_parity(jnp.concatenate([vlm, given], 0))
    pair = both(b, vlm, other[: vlm.shape[0]], 0)
    taken = jnp.concatenate(jnp.split(other[vlm.shape[0] :], folds, 1), 0)
    rows = both(b, kept, taken, 1)
    return jnp.concatenate([pair, action], 0), rows


def all_tokens(mine, n_vlm):
    h, c = lax.axis_index("h"), lax.axis_index("c")
    width = mine.shape[1]
    other = swap(mine, "h")
    two = both(h, mine[None], other[None], 0)
    theirs = swap(two, "c")
    four = jnp.stack([jnp.where(c == 0, two, theirs), jnp.where(c == 0, theirs, two)], 1)
    four = four.reshape(4, -1, width)
    normed_vlm = four[:, : 2 * n_vlm].reshape(4, 2, n_vlm, width).transpose(1, 0, 2, 3).reshape(-1, width)
    return normed_vlm, four[:, 2 * n_vlm :].reshape(-1, width)


def gelu(total):
    return total * 0.5 * (1.0 + lax.erf(total * 0.7071067811865476))


ROWS = 256


def weight_copies(place, core, slabs, weight, sems):
    x, w, c = (place[i] for i in range(3))
    part = slabs[0].shape[-1]
    copies = []
    for r, ref in enumerate(slabs):
        for q in range(4):
            col = lax.rem(x + jnp.where(c == 0, r, q), NX)
            row = lax.rem(w + jnp.where(c == 0, q, r), NW)
            columns = pl.ds(pl.multiple_of(lax.rem(row, 2) * part, part), part)
            for y in range(2):
                copies.append(
                    pltpu.make_async_copy(
                        ref.at[q, y, :, core],
                        weight.at[y, col, :, row // 2, :, columns],
                        sems.at[len(copies)],
                    )
                )
    return copies


def products(place, vlm, action, weight, store):
    depth, part = action.shape[1], weight.shape[-1] // 2
    columns = weight[...].reshape(depth, 2 * part)
    for i in range(0, action.shape[0], ROWS):
        total = jnp.dot(action[i : i + ROWS, :], columns, preferred_element_type=jnp.float32)
        values = gelu(total).astype(jnp.bfloat16)
        store(0, i, values[:, :part])
        store(1, i, values[:, part:])
    columns = weight[..., pl.ds(pl.multiple_of(lax.rem(place[1], 2) * part, part), part)].reshape(depth, part)
    for i in range(0, vlm.shape[0], ROWS):
        total = jnp.dot(vlm[i : i + ROWS, :], columns, preferred_element_type=jnp.float32)
        store(2, i, gelu(total).astype(jnp.bfloat16))


def column_copies(number, core, parts, vlm_out, action_out, sems):
    part = parts.shape[-1]
    starts = [pl.multiple_of((4 * b + 2 * core + number) * part, part) for b in (0, 1, 0)]
    return [
        pltpu.make_async_copy(parts.at[i], out.at[:, pl.ds(starts[i], part)], sems.at[i])
        for i, out in enumerate((action_out, action_out, vlm_out))
    ]


def part_kernel(number, given, own, n_in, place, vlm, action, *refs):
    slabs, refs = refs[:4], list(refs[n_in:])
    given_out = refs.pop(0) if given else None
    vlm_out, action_out = (refs.pop(0), refs.pop(0)) if own else (None, None)
    weights, stage, sems, out_sems = refs
    jobs = [1] * given + [0] * own
    copies = [weight_copies(place, core, slabs, weights.at[n], sems.at[n]) for n, core in enumerate(jobs)]
    for job in copies:
        for copy in job:
            copy.start()
    for n, core in enumerate(jobs):
        for copy in copies[n]:
            copy.wait()
        target = given_out if core else stage
        outs = [] if core else column_copies(number, place[2], stage, vlm_out, action_out, out_sems)

        def store(block, i, values, target=target, outs=outs):
            target[block, i : i + ROWS, :] = values
            if outs and i + ROWS == target.shape[1]:
                outs[block].start()

        products(place, vlm, action, weights.at[n], store)
        for copy in outs:
            copy.wait()


def merge_kernel(place, first, second, vlm_in, action_in, vlm_out, action_out, sems):
    del vlm_in, action_in
    copies = []
    for number, parts in enumerate((first, second)):
        copies += column_copies(number, 1 - place[2], parts, vlm_out, action_out, sems.at[number])
    for copy in copies:
        copy.start()
    for copy in copies:
        copy.wait()


SMEM = pl.BlockSpec(memory_space=pltpu.SMEM)
VMEM = pl.BlockSpec(memory_space=pltpu.VMEM)
HBM = pl.BlockSpec(memory_space=pltpu.HBM)


def outputs(vlm, action, slabs):
    place = jnp.stack([lax.axis_index(a) for a in "xwc"]).astype(jnp.int32)
    part, rows, count, depth = slabs[0][0].shape[-1], slabs[0][0].shape[-2], *action.shape
    taken = jax.ShapeDtypeStruct((3, count, part), jnp.bfloat16)
    wide = tuple(jax.ShapeDtypeStruct((count, n * part), jnp.bfloat16) for n in (4, 8))

    def call(number, given, own, before=()):
        jobs = given + own
        n_in = 4 + len(before)
        kernel = functools.partial(part_kernel, number, given, own, n_in)
        return pl.pallas_call(
            kernel,
            out_shape=(taken,) * given + wide * own,
            in_specs=[SMEM, VMEM, VMEM] + [HBM] * n_in,
            out_specs=(VMEM,) * given + (HBM, HBM) * own,
            scratch_shapes=[
                pltpu.VMEM((jobs, 2, NX, NU, 2, rows, 2 * part), jnp.bfloat16),
                pltpu.VMEM(taken.shape, taken.dtype),
                pltpu.SemaphoreType.DMA((jobs, 32)),
                pltpu.SemaphoreType.DMA((3,)),
            ],
            input_output_aliases={7 + i: given + i for i in range(len(before))},
            compiler_params=pltpu.CompilerParams(vmem_limit_bytes=14 * 1024 * 1024),
            cost_estimate=pl.CostEstimate(
                flops=6 * count * depth * part * jobs, bytes_accessed=6 * 1024 * 1024, transcendentals=0
            ),
        )(place, vlm, action, *slabs[number], *before)

    given_low, *wide_low = call(0, 1, 1)
    taken_low = swap(given_low, "c")
    (given_high,) = call(1, 1, 0)
    taken_high = swap(given_high, "c")
    wide_own = call(1, 0, 1, tuple(wide_low))
    return pl.pallas_call(
        merge_kernel,
        out_shape=wide,
        in_specs=[SMEM, VMEM, VMEM, HBM, HBM],
        out_specs=(HBM, HBM),
        scratch_shapes=[pltpu.SemaphoreType.DMA((2, 3))],
        input_output_aliases={3: 0, 4: 1},
        name="merge",
    )(place, taken_low, taken_high, *wide_own)


def local(vlm_tokens, action_tokens, norm_gain, proj_old):
    pieces = near_weight(proj_old)
    mine, proj_new = pair_exchange(vlm_tokens, action_tokens, norm_gain, proj_old)
    slabs = all_weight(pieces)
    vlm, action = all_tokens(mine, vlm_tokens.shape[0])
    vlm_hidden, action_hidden = outputs(vlm, action, slabs)
    return (vlm_hidden, action_hidden, proj_new)


def solution(mesh):
    finer = Mesh(mesh.devices.reshape(2, NX, NU, NW, 2, 2), ALL)
    dp, mp = ALL[:4], ALL[4:]
    in_specs = (P(ALL, None), P(ALL, None), P(), P(dp, mp))
    out_specs = (P(dp, mp), P(dp, mp), P(dp, mp))
    return jax.shard_map(local, mesh=finer, in_specs=in_specs, out_specs=out_specs, check_vma=False)
```

```python
import functools

import jax
import jax.numpy as jnp
from jax import lax
from jax.experimental import pallas as pl
from jax.experimental.pallas import tpu as pltpu
from jax.sharding import Mesh
from jax.sharding import PartitionSpec as P


ALL = ("y", "x", "u", "w", "h", "c")
NX, NU, NW = 4, 4, 4
PLANE = ("x", "u", "w", "c")

epsilon = 1e-06


def normalize(row_values, norm_gain):
    values = row_values.astype(jnp.float32)
    factor = lax.rsqrt(jnp.mean(values * values, axis=-1, keepdims=True) + epsilon)
    return (values * factor * norm_gain).astype(jnp.bfloat16)


def swap(array, axis):
    return lax.ppermute(array, axis, [(0, 1), (1, 0)])


def swap_parity(array):
    return lax.ppermute(array, "w", [(i, i ^ 1) for i in range(NW)])


def along(array, x_core, ahead):
    pairs = []
    for x in range(NX):
        for z in range(NU * NW):
            for c in range(2):
                sx, sz = ((x + ahead) % NX, z) if c == x_core else (x, (z + ahead) % (NU * NW))
                pairs.append(((sx * NU * NW + sz) * 2 + c, (x * NU * NW + z) * 2 + c))
    return lax.ppermute(array, PLANE, pairs)


def both(flag, own, other, dim):
    first = jnp.where(flag == 0, own, other)
    second = jnp.where(flag == 0, other, own)
    return jnp.concatenate([first, second], dim)


def near_weight(proj_old):
    c = lax.axis_index("c")
    half = proj_old.shape[1] // 2
    mine = lax.dynamic_slice_in_dim(proj_old, c * half, half, 1)
    given = lax.dynamic_slice_in_dim(proj_old, (1 - c) * half, half, 1)
    taken = swap(given, "c")
    mates = lax.all_gather(jnp.stack([mine, taken]), "u")
    planes = lax.all_gather(mates, "y")
    after, before = along(planes, 1, 1), along(planes, 1, -1)
    opposite = [along(planes[:1], 1, 2), along(planes[1:], 1, -2)]
    return [planes, after, jnp.concatenate(opposite, 0), before]


def all_weight(pieces):
    part = pieces[0].shape[-1] // 2
    low, high = (jnp.stack([p[..., i * part : (i + 1) * part] for p in pieces]) for i in range(2))
    low, high = lax.optimization_barrier((low, high))
    low_before = along(low, 0, -1)
    low_after = along(low, 0, 1)
    high_before = along(high, 0, -1)
    high_after = along(high, 0, 1)
    low_far = along(low_before, 0, -1)
    high_far = along(high_after, 0, 1)
    return (low, low_after, low_far, low_before), (high, high_after, high_far, high_before)


def pair_exchange(vlm_tokens, action_tokens, norm_gain, proj_old):
    b = lax.axis_index("w") % 2
    row_half, width = proj_old.shape[0] // 2, vlm_tokens.shape[1]
    vlm = normalize(vlm_tokens, norm_gain)
    action = normalize(action_tokens, norm_gain)
    kept = lax.dynamic_slice_in_dim(proj_old, b * row_half, row_half, 0)
    given = lax.dynamic_slice_in_dim(proj_old, (1 - b) * row_half, row_half, 0)
    folds = width // given.shape[1]
    given = jnp.concatenate(jnp.split(given, folds, 0), 1)
    other = swap_parity(jnp.concatenate([vlm, given], 0))
    pair = both(b, vlm, other[: vlm.shape[0]], 0)
    taken = jnp.concatenate(jnp.split(other[vlm.shape[0] :], folds, 1), 0)
    rows = both(b, kept, taken, 1)
    return jnp.concatenate([pair, action], 0), rows


def all_tokens(mine, n_vlm):
    h, c = lax.axis_index("h"), lax.axis_index("c")
    width = mine.shape[1]
    other = swap(mine, "h")
    two = both(h, mine[None], other[None], 0)
    theirs = swap(two, "c")
    four = jnp.stack([jnp.where(c == 0, two, theirs), jnp.where(c == 0, theirs, two)], 1)
    four = four.reshape(4, -1, width)
    normed_vlm = four[:, : 2 * n_vlm].reshape(4, 2, n_vlm, width).transpose(1, 0, 2, 3).reshape(-1, width)
    return normed_vlm, four[:, 2 * n_vlm :].reshape(-1, width)


def gelu(total):
    return total * 0.5 * (1.0 + lax.erf(total * 0.7071067811865476))


ROWS = 256


def weight_copies(place, core, slabs, weight, sems):
    x, w, c = (place[i] for i in range(3))
    part = slabs[0].shape[-1]
    copies = []
    for r, ref in enumerate(slabs):
        for q in range(4):
            col = lax.rem(x + jnp.where(c == 0, r, q), NX)
            row = lax.rem(w + jnp.where(c == 0, q, r), NW)
            columns = pl.ds(pl.multiple_of(lax.rem(row, 2) * part, part), part)
            for y in range(2):
                copies.append(
                    pltpu.make_async_copy(
                        ref.at[q, y, :, core],
                        weight.at[y, col, :, row // 2, :, columns],
                        sems.at[len(copies)],
                    )
                )
    return copies


def products(place, vlm, action, weight, store):
    depth, part = action.shape[1], weight.shape[-1] // 2
    columns = weight[...].reshape(depth, 2 * part)
    for i in range(0, action.shape[0], ROWS):
        total = jnp.dot(action[i : i + ROWS, :], columns, preferred_element_type=jnp.float32)
        values = gelu(total).astype(jnp.bfloat16)
        store(0, i, values[:, :part])
        store(1, i, values[:, part:])
    columns = weight[..., pl.ds(pl.multiple_of(lax.rem(place[1], 2) * part, part), part)].reshape(depth, part)
    for i in range(0, vlm.shape[0], ROWS):
        total = jnp.dot(vlm[i : i + ROWS, :], columns, preferred_element_type=jnp.float32)
        store(2, i, gelu(total).astype(jnp.bfloat16))


def column_copies(number, core, parts, vlm_out, action_out, sems):
    part = parts.shape[-1]
    starts = [pl.multiple_of((4 * b + 2 * core + number) * part, part) for b in (0, 1, 0)]
    return [
        pltpu.make_async_copy(parts.at[i], out.at[:, pl.ds(starts[i], part)], sems.at[i])
        for i, out in enumerate((action_out, action_out, vlm_out))
    ]


def part_kernel(number, given, own, n_in, place, vlm, action, *refs):
    slabs, before, refs = refs[:4], refs[4:n_in], list(refs[n_in:])
    given_out = refs.pop(0) if given else None
    vlm_out, action_out = (refs.pop(0), refs.pop(0)) if own else (None, None)
    weights, stage, sems, out_sems = refs
    more = column_copies(number - 1, 1 - place[2], before[0], vlm_out, action_out, out_sems.at[1]) if before else []
    for copy in more:
        copy.start()
    jobs = [1] * given + [0] * own
    copies = [weight_copies(place, core, slabs, weights.at[n], sems.at[n]) for n, core in enumerate(jobs)]
    for job in copies:
        for copy in job:
            copy.start()
    for n, core in enumerate(jobs):
        for copy in copies[n]:
            copy.wait()
        target = given_out if core else stage
        outs = [] if core else column_copies(number, place[2], stage, vlm_out, action_out, out_sems.at[0])

        def store(block, i, values, target=target, outs=outs):
            target[block, i : i + ROWS, :] = values
            if outs and i + ROWS == target.shape[1]:
                outs[block].start()

        products(place, vlm, action, weights.at[n], store)
        for copy in outs:
            copy.wait()
    for copy in more:
        copy.wait()


def merge_kernel(place, parts, vlm_in, action_in, vlm_out, action_out, sems):
    del vlm_in, action_in
    copies = column_copies(1, 1 - place[2], parts, vlm_out, action_out, sems)
    for copy in copies:
        copy.start()
    for copy in copies:
        copy.wait()


SMEM = pl.BlockSpec(memory_space=pltpu.SMEM)
VMEM = pl.BlockSpec(memory_space=pltpu.VMEM)
HBM = pl.BlockSpec(memory_space=pltpu.HBM)


def outputs(vlm, action, slabs):
    place = jnp.stack([lax.axis_index(a) for a in "xwc"]).astype(jnp.int32)
    part, rows, count, depth = slabs[0][0].shape[-1], slabs[0][0].shape[-2], *action.shape
    taken = jax.ShapeDtypeStruct((3, count, part), jnp.bfloat16)
    wide = tuple(jax.ShapeDtypeStruct((count, n * part), jnp.bfloat16) for n in (4, 8))

    def call(number, given, own, before=()):
        jobs = given + own
        n_in = 4 + len(before)
        kernel = functools.partial(part_kernel, number, given, own, n_in)
        return pl.pallas_call(
            kernel,
            out_shape=(taken,) * given + wide * own,
            in_specs=[SMEM, VMEM, VMEM] + [HBM] * 4 + [VMEM, HBM, HBM][: len(before)],
            out_specs=(VMEM,) * given + (HBM, HBM) * own,
            scratch_shapes=[
                pltpu.VMEM((jobs, 2, NX, NU, 2, rows, 2 * part), jnp.bfloat16),
                pltpu.VMEM(taken.shape, taken.dtype),
                pltpu.SemaphoreType.DMA((jobs, 32)),
                pltpu.SemaphoreType.DMA((2, 3)),
            ],
            input_output_aliases={7 + i: i - 1 for i in range(1, len(before))},
            compiler_params=pltpu.CompilerParams(vmem_limit_bytes=14 * 1024 * 1024),
            cost_estimate=pl.CostEstimate(
                flops=6 * count * depth * part * jobs, bytes_accessed=6 * 1024 * 1024, transcendentals=0
            ),
        )(place, vlm, action, *slabs[number], *before)

    given_low, *wide_low = call(0, 1, 1)
    taken_low = swap(given_low, "c")
    (given_high,) = call(1, 1, 0)
    taken_high = swap(given_high, "c")
    wide_own = call(1, 0, 1, (taken_low, *wide_low))
    return pl.pallas_call(
        merge_kernel,
        out_shape=wide,
        in_specs=[SMEM, VMEM, HBM, HBM],
        out_specs=(HBM, HBM),
        scratch_shapes=[pltpu.SemaphoreType.DMA((3,))],
        input_output_aliases={2: 0, 3: 1},
        name="merge",
    )(place, taken_high, *wide_own)


def local(vlm_tokens, action_tokens, norm_gain, proj_old):
    pieces = near_weight(proj_old)
    mine, proj_new = pair_exchange(vlm_tokens, action_tokens, norm_gain, proj_old)
    slabs = all_weight(pieces)
    vlm, action = all_tokens(mine, vlm_tokens.shape[0])
    vlm_hidden, action_hidden = outputs(vlm, action, slabs)
    return (vlm_hidden, action_hidden, proj_new)


def solution(mesh):
    finer = Mesh(mesh.devices.reshape(2, NX, NU, NW, 2, 2), ALL)
    dp, mp = ALL[:4], ALL[4:]
    in_specs = (P(ALL, None), P(ALL, None), P(), P(dp, mp))
    out_specs = (P(dp, mp), P(dp, mp), P(dp, mp))
    return jax.shard_map(local, mesh=finer, in_specs=in_specs, out_specs=out_specs, check_vma=False)
```

```python
import functools

import jax
import jax.numpy as jnp
from jax import lax
from jax.experimental import pallas as pl
from jax.experimental.pallas import tpu as pltpu
from jax.sharding import Mesh
from jax.sharding import PartitionSpec as P


ALL = ("y", "x", "u", "w", "h", "c")
NX, NU, NW = 4, 4, 4
PLANE = ("x", "u", "w", "c")

epsilon = 1e-06


def normalize(row_values, norm_gain):
    values = row_values.astype(jnp.float32)
    factor = lax.rsqrt(jnp.mean(values * values, axis=-1, keepdims=True) + epsilon)
    return (values * factor * norm_gain).astype(jnp.bfloat16)


def swap(array, axis):
    return lax.ppermute(array, axis, [(0, 1), (1, 0)])


def swap_parity(array):
    return lax.ppermute(array, "w", [(i, i ^ 1) for i in range(NW)])


def along(array, x_core, ahead):
    pairs = []
    for x in range(NX):
        for z in range(NU * NW):
            for c in range(2):
                sx, sz = ((x + ahead) % NX, z) if c == x_core else (x, (z + ahead) % (NU * NW))
                pairs.append(((sx * NU * NW + sz) * 2 + c, (x * NU * NW + z) * 2 + c))
    return lax.ppermute(array, PLANE, pairs)


def both(flag, own, other, dim):
    first = jnp.where(flag == 0, own, other)
    second = jnp.where(flag == 0, other, own)
    return jnp.concatenate([first, second], dim)


def near_weight(proj_old, outgoing):
    c = lax.axis_index("c")
    half = proj_old.shape[1] // 2
    mine = lax.dynamic_slice_in_dim(proj_old, c * half, half, 1)
    given = lax.dynamic_slice_in_dim(proj_old, (1 - c) * half, half, 1)
    taken = swap(given, "c")
    mates = lax.all_gather(jnp.stack([mine, taken]), "u")
    mates, outgoing = lax.optimization_barrier((mates, outgoing))
    incoming = swap_parity(outgoing)
    planes = lax.all_gather(mates, "y")
    after, before = along(planes, 1, 1), along(planes, 1, -1)
    opposite = [along(planes[:1], 1, 2), along(planes[1:], 1, -2)]
    return [planes, after, jnp.concatenate(opposite, 0), before], incoming


def all_weight(pieces):
    part = pieces[0].shape[-1] // 2
    low, high = (jnp.stack([p[..., i * part : (i + 1) * part] for p in pieces]) for i in range(2))
    low, high = lax.optimization_barrier((low, high))
    low_before = along(low, 0, -1)
    low_after = along(low, 0, 1)
    high_before = along(high, 0, -1)
    high_after = along(high, 0, 1)
    low_far = along(low_before, 0, -1)
    high_far = along(high_after, 0, 1)
    return (low, low_after, low_far, low_before), (high, high_after, high_far, high_before)


def for_neighbour(vlm_tokens, norm_gain, proj_old):
    row_half, width = proj_old.shape[0] // 2, vlm_tokens.shape[1]
    vlm = normalize(vlm_tokens, norm_gain)
    b = lax.axis_index("w") % 2
    given = lax.dynamic_slice_in_dim(proj_old, (1 - b) * row_half, row_half, 0)
    given = jnp.concatenate(jnp.split(given, width // given.shape[1], 0), 1)
    return jnp.concatenate([vlm, given], 0)


def with_neighbour(outgoing, incoming, action_tokens, norm_gain, proj_old):
    b = lax.axis_index("w") % 2
    row_half, width = proj_old.shape[0] // 2, outgoing.shape[1]
    folds = width // proj_old.shape[1]
    count = outgoing.shape[0] - row_half // folds
    action = normalize(action_tokens, norm_gain)
    tokens = jnp.concatenate([both(b, outgoing[:count], incoming[:count], 0), action], 0)
    kept = lax.dynamic_slice_in_dim(proj_old, b * row_half, row_half, 0)
    taken = jnp.concatenate(jnp.split(incoming[count:], folds, 1), 0)
    rows = both(b, kept, taken, 1)
    return tokens, rows


def all_tokens(mine, n_vlm):
    h, c = lax.axis_index("h"), lax.axis_index("c")
    width = mine.shape[1]
    other = swap(mine, "h")
    two = both(h, mine[None], other[None], 0)
    theirs = swap(two, "c")
    four = jnp.stack([jnp.where(c == 0, two, theirs), jnp.where(c == 0, theirs, two)], 1)
    four = four.reshape(4, -1, width)
    normed_vlm = four[:, : 2 * n_vlm].reshape(4, 2, n_vlm, width).transpose(1, 0, 2, 3).reshape(-1, width)
    return normed_vlm, four[:, 2 * n_vlm :].reshape(-1, width)


def gelu(total):
    return total * 0.5 * (1.0 + lax.erf(total * 0.7071067811865476))


ROWS = 256


def weight_copies(place, core, slabs, weight, sems):
    x, w, c = (place[i] for i in range(3))
    part = slabs[0].shape[-1]
    copies = []
    for r, ref in enumerate(slabs):
        for q in range(4):
            col = lax.rem(x + jnp.where(c == 0, r, q), NX)
            row = lax.rem(w + jnp.where(c == 0, q, r), NW)
            columns = pl.ds(pl.multiple_of(lax.rem(row, 2) * part, part), part)
            for y in range(2):
                copies.append(
                    pltpu.make_async_copy(
                        ref.at[q, y, :, core],
                        weight.at[y, col, :, row // 2, :, columns],
                        sems.at[len(copies)],
                    )
                )
    return copies


def products(place, vlm, action, weight, store):
    depth, part = action.shape[1], weight.shape[-1] // 2
    columns = weight[...].reshape(depth, 2 * part)
    for i in range(0, action.shape[0], ROWS):
        total = jnp.dot(action[i : i + ROWS, :], columns, preferred_element_type=jnp.float32)
        values = gelu(total).astype(jnp.bfloat16)
        store(0, i, values[:, :part])
        store(1, i, values[:, part:])
    columns = weight[..., pl.ds(pl.multiple_of(lax.rem(place[1], 2) * part, part), part)].reshape(depth, part)
    for i in range(0, vlm.shape[0], ROWS):
        total = jnp.dot(vlm[i : i + ROWS, :], columns, preferred_element_type=jnp.float32)
        store(2, i, gelu(total).astype(jnp.bfloat16))


def column_copies(number, core, parts, vlm_out, action_out, sems):
    part = parts.shape[-1]
    starts = [pl.multiple_of((4 * b + 2 * core + number) * part, part) for b in (0, 1, 0)]
    return [
        pltpu.make_async_copy(parts.at[i], out.at[:, pl.ds(starts[i], part)], sems.at[i])
        for i, out in enumerate((action_out, action_out, vlm_out))
    ]


def part_kernel(number, given, own, n_in, place, vlm, action, *refs):
    slabs, before, refs = refs[:4], refs[4:n_in], list(refs[n_in:])
    given_out = refs.pop(0) if given else None
    vlm_out, action_out = (refs.pop(0), refs.pop(0)) if own else (None, None)
    weights, stage, sems, out_sems = refs
    more = column_copies(number - 1, 1 - place[2], before[0], vlm_out, action_out, out_sems.at[1]) if before else []
    for copy in more:
        copy.start()
    jobs = [1] * given + [0] * own
    copies = [weight_copies(place, core, slabs, weights.at[n], sems.at[n]) for n, core in enumerate(jobs)]
    for job in copies:
        for copy in job:
            copy.start()
    for n, core in enumerate(jobs):
        for copy in copies[n]:
            copy.wait()
        target = given_out if core else stage
        outs = [] if core else column_copies(number, place[2], stage, vlm_out, action_out, out_sems.at[0])

        def store(block, i, values, target=target, outs=outs):
            target[block, i : i + ROWS, :] = values
            if outs and i + ROWS == target.shape[1]:
                outs[block].start()

        products(place, vlm, action, weights.at[n], store)
        for copy in outs:
            copy.wait()
    for copy in more:
        copy.wait()


def merge_kernel(place, parts, vlm_in, action_in, vlm_out, action_out, sems):
    del vlm_in, action_in
    copies = column_copies(1, 1 - place[2], parts, vlm_out, action_out, sems)
    for copy in copies:
        copy.start()
    for copy in copies:
        copy.wait()


SMEM = pl.BlockSpec(memory_space=pltpu.SMEM)
VMEM = pl.BlockSpec(memory_space=pltpu.VMEM)
HBM = pl.BlockSpec(memory_space=pltpu.HBM)


def outputs(vlm, action, slabs):
    place = jnp.stack([lax.axis_index(a) for a in "xwc"]).astype(jnp.int32)
    part, rows, count, depth = slabs[0][0].shape[-1], slabs[0][0].shape[-2], *action.shape
    taken = jax.ShapeDtypeStruct((3, count, part), jnp.bfloat16)
    wide = tuple(jax.ShapeDtypeStruct((count, n * part), jnp.bfloat16) for n in (4, 8))

    def call(number, given, own, before=()):
        jobs = given + own
        n_in = 4 + len(before)
        kernel = functools.partial(part_kernel, number, given, own, n_in)
        return pl.pallas_call(
            kernel,
            out_shape=(taken,) * given + wide * own,
            in_specs=[SMEM, VMEM, VMEM] + [HBM] * 4 + [VMEM, HBM, HBM][: len(before)],
            out_specs=(VMEM,) * given + (HBM, HBM) * own,
            scratch_shapes=[
                pltpu.VMEM((jobs, 2, NX, NU, 2, rows, 2 * part), jnp.bfloat16),
                pltpu.VMEM(taken.shape, taken.dtype),
                pltpu.SemaphoreType.DMA((jobs, 32)),
                pltpu.SemaphoreType.DMA((2, 3)),
            ],
            input_output_aliases={7 + i: i - 1 for i in range(1, len(before))},
            compiler_params=pltpu.CompilerParams(vmem_limit_bytes=14 * 1024 * 1024),
            cost_estimate=pl.CostEstimate(
                flops=6 * count * depth * part * jobs, bytes_accessed=6 * 1024 * 1024, transcendentals=0
            ),
        )(place, vlm, action, *slabs[number], *before)

    given_low, *wide_low = call(0, 1, 1)
    taken_low = swap(given_low, "c")
    (given_high,) = call(1, 1, 0)
    taken_high = swap(given_high, "c")
    wide_own = call(1, 0, 1, (taken_low, *wide_low))
    return pl.pallas_call(
        merge_kernel,
        out_shape=wide,
        in_specs=[SMEM, VMEM, HBM, HBM],
        out_specs=(HBM, HBM),
        scratch_shapes=[pltpu.SemaphoreType.DMA((3,))],
        input_output_aliases={2: 0, 3: 1},
        name="merge",
    )(place, taken_high, *wide_own)


def local(vlm_tokens, action_tokens, norm_gain, proj_old):
    outgoing = for_neighbour(vlm_tokens, norm_gain, proj_old)
    pieces, incoming = near_weight(proj_old, outgoing)
    mine, proj_new = with_neighbour(outgoing, incoming, action_tokens, norm_gain, proj_old)
    slabs = all_weight(pieces)
    vlm, action = all_tokens(mine, vlm_tokens.shape[0])
    vlm_hidden, action_hidden = outputs(vlm, action, slabs)
    return (vlm_hidden, action_hidden, proj_new)


def solution(mesh):
    finer = Mesh(mesh.devices.reshape(2, NX, NU, NW, 2, 2), ALL)
    dp, mp = ALL[:4], ALL[4:]
    in_specs = (P(ALL, None), P(ALL, None), P(), P(dp, mp))
    out_specs = (P(dp, mp), P(dp, mp), P(dp, mp))
    return jax.shard_map(local, mesh=finer, in_specs=in_specs, out_specs=out_specs, check_vma=False)
```
